32 devices in a mesh: front: 4 (over z), blk: 8 (over y, x, core).
Axes of the slice: x: 2, y: 2, z: 4, core: 2. Of those that a mesh axis runs over, the one named last changes fastest.
Arguments:
- panel_column: bfloat16 [4, 4096, 256], P('front', 'blk'), may hold values from -6 to 6
- upper_inverse: bfloat16 [4, 256, 256], P('front'), may hold values from -0.375 to 0.375
- panel_rows: bfloat16 [4, 256, 12288], P('front', None, 'blk'), may hold values from -0.375 to 0.375
- trailing: bfloat16 [4, 4096, 12288], P('front', 'blk')
- sketch: bfloat16 [12288, 256], replicated, may hold values from -0.0546875 to 0.0546875
- row_map: int32 [4, 16, 256], P('front', 'blk'), may hold values from 0 to 255, each once within a row
- parent_block: int32 [4, 16], replicated, may hold values from 0 to 23, as said below
- parent_slot: int32 [24], replicated, may hold values from 0 to 31, as said below
Outputs:
- factored_column: bfloat16 [4, 4096, 256], P('front', 'blk')
- right_factor: bfloat16 [4, 12288, 256], P('front', 'blk')
- parent_left: bfloat16 [8192, 1024], P(('front', 'blk'))
The draws below stay inside these ranges and needn't reach their ends.
Inputs may be any that keep to these rules, and one draw needn't show every extreme that they name: `parent_block`: within one front the 16 blocks go to distinct parent blocks; some parent block receives a block of every front. `parent_slot`: distinct values: a device owns at most one parent block.
All inputs are finite; a program needn't handle non-finite values.
Results may differ from the reference program's by a relative error of at most 0.0095.
Values may be sent and summed in bfloat16 or wider, within the bound.
No kernel may reach another device: no remote copies, remote signals or barrier semaphores. Data moves between devices by JAX's collectives and lax.ppermute only.
A program may use at most 128 MiB of HBM per device.

```python
import math
import jax
import jax.numpy as jnp
from jax import lax

BLOCK = 256
PANEL = 256
RANK = 256
COLS = 12288
FRONTS = 4
SLAB = 4096
NB = 16
PBLOCKS = 24
N_FRONT = 4
N_BLK = 8


def draw_trailing(key, part):
    seed_key = jax.random.fold_in(key, 11)
    entry_key, row_key, col_key = jax.random.split(seed_key, 3)
    shape = (FRONTS, SLAB, COLS)
    entries = jax.random.normal(entry_key, shape, jnp.float32)
    growth = 3.0
    position = jnp.arange(SLAB, dtype=jnp.float32) / SLAB
    row_scale = 10.0 ** jax.random.uniform(row_key, (FRONTS, SLAB, 1), jnp.float32, -0.5, 0.5)
    row_scale = row_scale * growth ** (position[None, :, None] - 0.5)
    col_scale = 10.0 ** jax.random.uniform(col_key, (1, 1, COLS), jnp.float32, -0.5, 0.5)
    return (entries * row_scale * col_scale).astype(jnp.bfloat16)


def draw_parent_block(key, part):
    seed_key = jax.random.fold_in(key, 23)

    def pick_front(front_number):
        front_key = jax.random.fold_in(seed_key, front_number)
        first_key, second_key = jax.random.split(front_key)
        others = jax.random.permutation(first_key, PBLOCKS - 1)[:NB - 1].astype(jnp.int32) + 1
        chosen = jnp.concatenate([jnp.zeros((1,), jnp.int32), others])
        return jax.random.permutation(second_key, chosen)
    return jax.vmap(pick_front)(jnp.arange(FRONTS, dtype=jnp.int32)).astype(jnp.int32)


def draw_parent_slot(key, part):
    seed_key = jax.random.fold_in(key, 37)
    return jax.random.permutation(seed_key, N_FRONT * N_BLK)[:PBLOCKS].astype(jnp.int32)


def block_levels(own_key, shape, cuts, smallest, high):
    def one(axis_at, blocks):
        draws = jax.random.uniform(jax.random.fold_in(jax.random.fold_in(own_key, 6), axis_at), (blocks,), jnp.float32, smallest / len(cuts), high / len(cuts))
        return jnp.repeat(jnp.exp(draws), shape[axis_at] // blocks).reshape((-1,) + (1,) * (len(shape) - axis_at - 1))

    loudness = one(*cuts[0])
    for cut in cuts[1:]:
        loudness = loudness * one(*cut)
    return loudness


def gaussian(rng, extent, spread, most, shards=(), held_as=jnp.bfloat16):
    factor_of = block_levels(rng, extent, shards, -0.22, 0.18) if shards else 1.0
    values = jax.random.normal(rng, extent, jnp.float32) * spread * factor_of
    return jnp.minimum(jnp.maximum(values, -most), most).astype(held_as)


def setup_inputs(seed: int = 0) -> dict:
    streams_of = jax.random.split(jax.random.key(seed), 9)
    panel_column = gaussian(streams_of[0], (FRONTS, SLAB, PANEL), 1.0, 6.0, ((0, 4), (1, 8)))
    upper_inverse = gaussian(streams_of[1], (FRONTS, PANEL, PANEL), PANEL ** -0.5, 0.375, ((0, 4),))
    panel_rows = gaussian(streams_of[2], (FRONTS, PANEL, COLS), PANEL ** -0.5, 0.375, ((0, 4), (2, 8)))
    trailing = draw_trailing(jax.random.fold_in(streams_of[8], 71), 0)
    sketch = gaussian(streams_of[4], (COLS, RANK), COLS ** -0.5, 0.0546875)
    row_map = jax.vmap(lambda own: jax.random.permutation(own, BLOCK))(jax.random.split(streams_of[5], FRONTS * NB)).reshape((FRONTS, NB, BLOCK)).astype(jnp.int32)
    parent_block = draw_parent_block(jax.random.fold_in(streams_of[8], 71), 0)
    parent_slot = draw_parent_slot(jax.random.fold_in(streams_of[8], 71), 0)
    return {"panel_column": panel_column, "upper_inverse": upper_inverse, "panel_rows": panel_rows, "trailing": trailing, "sketch": sketch, "row_map": row_map, "parent_block": parent_block, "parent_slot": parent_slot}


def reference(panel_column, upper_inverse, panel_rows, trailing, sketch, row_map, parent_block, parent_slot):
    global_sketch = sketch

    def per_front(operands):
        column, inverse, pivot_rows, trail = operands
        factored = jnp.dot(column.astype(jnp.float32), inverse.astype(jnp.float32), preferred_element_type=jnp.float32).astype(jnp.bfloat16)
        updated = (trail.astype(jnp.float32) - jnp.dot(factored.astype(jnp.float32), pivot_rows.astype(jnp.float32), preferred_element_type=jnp.float32)).astype(jnp.bfloat16)
        sketched = jnp.dot(updated.astype(jnp.float32), global_sketch.astype(jnp.float32), preferred_element_type=jnp.float32).astype(jnp.bfloat16)
        gram_matrix = jnp.dot(sketched.T.astype(jnp.float32), sketched.astype(jnp.float32), preferred_element_type=jnp.float32) / SLAB
        factor_low = jnp.linalg.cholesky(gram_matrix)
        basis_rows = jax.scipy.linalg.solve_triangular(factor_low, sketched.astype(jnp.float32).T, lower=True).T
        cross_terms = jnp.dot(updated.T.astype(jnp.float32), sketched.astype(jnp.float32), preferred_element_type=jnp.float32)
        right_rows = jax.scipy.linalg.solve_triangular(factor_low, cross_terms.T, lower=True).T / math.sqrt(SLAB)
        return (factored, right_rows.astype(jnp.bfloat16), basis_rows.astype(jnp.bfloat16))
    factored_column, right_factor, left_factor = lax.map(per_front, (panel_column, upper_inverse, panel_rows, trailing))
    owner_index = parent_slot[parent_block]
    row_target = (owner_index[:, :, None] * BLOCK + row_map).reshape(FRONTS, SLAB).astype(jnp.int32)
    front_column = jnp.broadcast_to(jnp.arange(FRONTS, dtype=jnp.int32)[:, None], (FRONTS, SLAB))
    parent_rows = jnp.zeros((N_FRONT * N_BLK * BLOCK, FRONTS, RANK), left_factor.dtype)
    parent_rows = parent_rows.at[row_target, front_column].set(left_factor)
    parent_left = parent_rows.reshape(N_FRONT * N_BLK * BLOCK, FRONTS * RANK)
    return (factored_column, right_factor, parent_left)
```

```python
import functools
import math

import jax
import jax.numpy as jnp
from jax import lax
from jax.experimental import pallas as pl
from jax.experimental.pallas import tpu as pltpu
from jax.sharding import PartitionSpec as P


F32 = jnp.float32
BF16 = jnp.bfloat16


def fdot(a, b):
    return jnp.dot(a, b, preferred_element_type=F32)


def split_two(x):
    high = x.astype(BF16)
    return high, (x - high.astype(F32)).astype(BF16)


def dot_three(a, b):
    a_high, a_low = split_two(a)
    b_high, b_low = split_two(b)
    return fdot(a_high, b_high) + (fdot(a_high, b_low) + fdot(a_low, b_high))


VMEM = pltpu.VMEM
SMEM = pltpu.SMEM
HBM = pltpu.MemorySpace.HBM


def specs(spaces):
    return [pl.BlockSpec(memory_space=space) for space in spaces]


def local_call(kernel, spaces, out_shape, out_spaces, limit=8, **options):
    return pl.pallas_call(
        kernel,
        in_specs=specs(spaces),
        out_specs=specs(out_spaces),
        out_shape=out_shape,
        compiler_params=pltpu.CompilerParams(vmem_limit_bytes=limit << 20),
        **options,
    )


def in_hbm(x):
    return pltpu.with_memory_space_constraint(x, HBM)


def sketch_kernel(first, count, t_hbm, s_hbm, a_ref, b_ref, *refs):
    out_refs, (t_ref, s_ref, sems) = refs[:-3], refs[-3:]
    step = t_ref.shape[1] // count
    copies = []
    for i in range(count):
        near = pl.ds(i * step, step)
        far = pl.ds((first + i) * step, step)
        pair = (
            pltpu.make_async_copy(t_hbm.at[:, far], t_ref.at[:, near], sems.at[0, i]),
            pltpu.make_async_copy(s_hbm.at[far, :], s_ref.at[near, :], sems.at[1, i]),
        )
        for copy in pair:
            copy.start()
        copies.append(pair)
    if first == 0:
        factored = fdot(a_ref[...], b_ref[...]).astype(BF16)
        out_refs[1][...] = factored
        out_refs[2][...] = factored
    else:
        out_refs[0][...] = a_ref[...]
    for i in range(count):
        near = pl.ds(i * step, step)
        for copy in copies[i]:
            copy.wait()
        part = fdot(t_ref[:, near], s_ref[near, :])
        if first + i == 0:
            out_refs[0][...] = part
        else:
            out_refs[0][...] += part


def sketch_part(first, count, chunks, trail, sketch, a, b):
    rows, cols = trail.shape
    rank = sketch.shape[1]
    out_shape = [jax.ShapeDtypeStruct((rows, rank), F32)]
    if first == 0:
        out_shape += [jax.ShapeDtypeStruct((rows, b.shape[1]), BF16)] * 2
    span = cols // chunks * count
    return local_call(
        functools.partial(sketch_kernel, first, count),
        [HBM, HBM, VMEM, VMEM],
        out_shape,
        [VMEM] * len(out_shape),
        limit=24,
        scratch_shapes=[
            pltpu.VMEM((rows, span), BF16),
            pltpu.VMEM((span, rank), BF16),
            pltpu.SemaphoreType.DMA((2, count)),
        ],
    )(in_hbm(trail), in_hbm(sketch), a, b)


def in_order(core, mine, other):
    first = core == 0
    return jnp.where(first, mine, other), jnp.where(first, other, mine)


def finish_kernel(
    ts_ref, f_ref, mine_ref, other_ref, sk_ref, skt_ref, away_ref, keep_ref, work
):
    core = lax.axis_index("blk") % 2
    factored = f_ref[...]
    half = mine_ref.shape[0]
    value = ts_ref[...]
    for k, part in enumerate(in_order(core, mine_ref[...], other_ref[...])):
        high, low = split_two(part)
        columns = factored[:, k * half : (k + 1) * half]
        value = value - (fdot(columns, high) + fdot(columns, low))
    sketched = value.astype(BF16)
    sk_ref[...] = sketched
    turned = sketched.T
    skt_ref[...] = turned
    rank = sketched.shape[1]
    work[:, :rank] = fdot(turned, sketched)
    work[:, rank:] = fdot(turned, factored)
    rows = keep_ref.shape[0]
    keep_ref[...] = work[pl.ds(pl.multiple_of(core * rows, rows), rows), :]
    away_ref[...] = work[pl.ds(pl.multiple_of((1 - core) * rows, rows), rows), :]


def finish_sketch(ts, factored, mine, other):
    rows, rank = ts.shape
    wide = rank + factored.shape[1]
    return local_call(
        finish_kernel,
        [VMEM] * 4,
        [
            jax.ShapeDtypeStruct((rows, rank), BF16),
            jax.ShapeDtypeStruct((rank, rows), BF16),
            jax.ShapeDtypeStruct((rank // 2, wide), F32),
            jax.ShapeDtypeStruct((rank // 2, wide), F32),
        ],
        [VMEM] * 4,
        scratch_shapes=[pltpu.VMEM((rank, wide), F32)],
    )(ts, factored, mine, other)


def bit_of(me, mask):
    return (me // mask) % 2


def owners(me, order, stage):
    rest = order[stage + 1 :]
    base = sum(bit_of(me, mask) * mask for mask in order[:stage])
    if stage < len(order):
        base = base + (1 - bit_of(me, order[stage])) * order[stage]
    return [
        base + sum(((i >> (len(rest) - 1 - k)) & 1) * mask for k, mask in enumerate(rest))
        for i in range(1 << len(rest))
    ]


def row_base(me, order, stage, earlier):
    base = 0
    for k in range(earlier + 1, min(stage + 1, len(order))):
        bit = bit_of(me, order[k])
        base = base * 2 + (bit if k < stage else 1 - bit)
    return base * (1 << max(len(order) - stage - 1, 0))


def share_kernel(jobs, colours, skt_ref, t_hbm, *refs):
    out_refs, (t_ref, sems) = refs[: len(jobs)], refs[len(jobs) :]
    me = lax.axis_index("blk")
    width = t_ref.shape[2]
    places = []
    for out_ref, (colour, order, stage) in zip(out_refs, jobs):
        for i, owner in enumerate(owners(me, order, stage)):
            places.append((out_ref, i, owner * colours + colour))
    copies = []
    for i, (_, _, place) in enumerate(places):
        span = pl.ds(pl.multiple_of(place * width, width), width)
        copies.append(pltpu.make_async_copy(t_hbm.at[:, span], t_ref.at[i], sems.at[i]))
        copies[-1].start()
    turned = skt_ref[...]
    for i, (out_ref, at, _) in enumerate(places):
        copies[i].wait()
        out_ref[at] = fdot(turned, t_ref[i]).astype(out_ref.dtype)


def share_product(jobs, colours, skt, trail, width, dtype):
    rank, rows = skt.shape
    numbers = [1 << max(len(order) - stage - 1, 0) for _, order, stage in jobs]
    return local_call(
        functools.partial(share_kernel, jobs, colours),
        [VMEM, HBM],
        [jax.ShapeDtypeStruct((number, rank, width), dtype) for number in numbers],
        [VMEM] * len(jobs),
        limit=28,
        scratch_shapes=[
            pltpu.VMEM((sum(numbers), rows, width), BF16),
            pltpu.SemaphoreType.DMA((sum(numbers),)),
        ],
    )(skt, in_hbm(trail))


def merge_kernel(order, stage, share_ref, *refs):
    received, out_ref = refs[:-1], refs[-1]
    me = lax.axis_index("blk")
    for i in range(out_ref.shape[0]):
        total = share_ref[i]
        for t, ref in enumerate(received):
            total = total + ref[row_base(me, order, stage, t) + i].astype(F32)
        out_ref[i] = total.astype(out_ref.dtype)


def merge(order, stage, share, received):
    return local_call(
        functools.partial(merge_kernel, order, stage),
        [VMEM] * (1 + len(received)),
        [jax.ShapeDtypeStruct(share.shape, BF16)],
        [VMEM],
    )(share, *received)[0]


def early_kernel(orders, w_ref, wh_ref, p_ref, *refs):
    out_ref = refs[-1]
    me = lax.axis_index("blk")
    w_high, w_low = split_two(w_ref[...])
    wh_high, wh_low = split_two(wh_ref[...])
    at = 0
    for colour, order in enumerate(orders):
        width = refs[at].shape[2]
        total = refs[at][0]
        for t in range(len(order) - 1):
            total = total + refs[at + 1 + t][row_base(me, order, len(order), t)].astype(F32)
        at += len(order)
        high, low = split_two(total)
        own = p_ref[:, colour * width : (colour + 1) * width]
        value = fdot(w_high, high) + (fdot(w_high, low) + fdot(w_low, high))
        out_ref[colour] = value - (fdot(wh_high, own) + fdot(wh_low, own))


def right_early(orders, w, wh, panel, shares, received):
    flat = []
    for share, group in zip(shares, received):
        flat += [share] + list(group)
    rank, width = shares[0].shape[1:]
    return local_call(
        functools.partial(early_kernel, orders),
        [VMEM] * (3 + len(flat)),
        [jax.ShapeDtypeStruct((len(orders), rank, width), F32)],
        [VMEM],
        limit=16,
    )(w, wh, panel, *flat)[0]


def late_kernel(scale, w_ref, early_ref, *refs):
    last, out_ref = refs[:-1], refs[-1]
    width = early_ref.shape[2]
    w_high, w_low = split_two(w_ref[...])
    for colour, ref in enumerate(last):
        got = ref[0]
        value = early_ref[colour] + (fdot(w_high, got) + fdot(w_low, got))
        out_ref[colour * width : (colour + 1) * width, :] = (value * scale).astype(BF16).T


def right_late(w, early, last, scale):
    colours, rank, width = early.shape
    return local_call(
        functools.partial(late_kernel, scale),
        [VMEM] * (2 + len(last)),
        [jax.ShapeDtypeStruct((colours * width, rank), BF16)],
        [VMEM],
    )(w, early, *last)[0]


def spread_kernel(sk_ref, map_ref, keep_ref, send_ref, work):
    pieces, blocks, piece, _ = work.shape
    rows = pieces * piece
    me = lax.axis_index("blk")
    position = lax.broadcasted_iota(jnp.int32, (rows, rows), 0)
    for b in range(blocks):
        pick = (map_ref[b : b + 1, :] == position).astype(F32).astype(BF16)
        placed = fdot(pick, sk_ref[b * rows : (b + 1) * rows, :]).astype(BF16)
        for c in range(pieces):
            work[c, b] = placed[c * piece : (c + 1) * piece, :]
    half = pieces // 2
    for m in range(half):
        keep_ref[m] = work[jnp.bitwise_xor(me, m)]
        send_ref[m] = work[jnp.bitwise_xor(me, m + half)]


def spread_rows(sketched, row_map, pieces):
    blocks, rows = row_map.shape
    shape = (blocks, rows // pieces, sketched.shape[1])
    return local_call(
        spread_kernel,
        [VMEM, VMEM],
        [jax.ShapeDtypeStruct((pieces // 2,) + shape, BF16)] * 2,
        [VMEM] * 2,
        scratch_shapes=[pltpu.VMEM((pieces,) + shape, BF16)],
    )(sketched, row_map)


def regroup_kernel(*refs):
    keep_ref, came_ref, next_ref, send_ref = refs
    half = keep_ref.shape[0] // 2
    sources = keep_ref.shape[1]
    for m in range(half):
        for k, ref in enumerate((keep_ref, came_ref)):
            next_ref[m, k * sources : (k + 1) * sources] = ref[m]
            send_ref[m, k * sources : (k + 1) * sources] = ref[m + half]


def regroup(keep, came):
    half, sources = keep.shape[0] // 2, 2 * keep.shape[1]
    shape = jax.ShapeDtypeStruct((half, sources) + keep.shape[2:], BF16)
    return local_call(regroup_kernel, [VMEM] * 2, [shape] * 2, [VMEM] * 2)(keep, came)


def route_kernel(source_ref, w_ref, *refs):
    spread, (out_ref, work) = refs[:-2], refs[-2:]
    _, blocks, piece, rank = spread[0].shape
    w_high, w_low = split_two(w_ref[...])
    rows = jnp.concatenate([ref[0].reshape(blocks * piece, rank) for ref in spread], axis=0)
    across = (((1,), (1,)), ((), ()))
    value = lax.dot_general(rows, w_high, across, preferred_element_type=F32)
    value = value + lax.dot_general(rows, w_low, across, preferred_element_type=F32)
    work[0] = jnp.zeros((piece, rank), BF16)
    for b in range(blocks * len(spread)):
        work[1 + b] = value[b * piece : (b + 1) * piece, :].astype(BF16)

    def move(d, carry):
        out_ref[d] = work[source_ref[d]]
        return carry

    lax.fori_loop(0, out_ref.shape[0], move, 0, unroll=4)


def route_left(source, spread, w):
    _, blocks, piece, rank = spread[0].shape
    return local_call(
        route_kernel,
        [SMEM, VMEM] + [VMEM] * len(spread),
        [jax.ShapeDtypeStruct((source.shape[0], piece, rank), BF16)],
        [VMEM],
        scratch_shapes=[pltpu.VMEM((blocks * len(spread) + 1, piece, rank), BF16)],
    )(source, w, *spread)[0]


def gather_kernel(x_ref, out_ref):
    devices, piece, rank = x_ref.shape
    pieces = out_ref.shape[0] // piece
    for d in range(devices):
        f, c = d // pieces, d % pieces
        out_ref[c * piece : (c + 1) * piece, f * rank : (f + 1) * rank] = x_ref[d]


def gather_left(x, fronts):
    devices, piece, rank = x.shape
    return local_call(
        gather_kernel,
        [VMEM],
        [jax.ShapeDtypeStruct((devices // fronts * piece, fronts * rank), BF16)],
        [VMEM],
    )(x)[0]


TILE = 8
LANES = 128


def eliminate(tiles, pivots):
    tiles = list(tiles)
    count = len(tiles)
    row = lax.broadcasted_iota(jnp.int32, (TILE, LANES), 0)
    group = TILE
    for start in range(0, pivots, group):
        home = start // TILE
        at = start % TILE
        col = [
            {
                t: jnp.broadcast_to(tiles[t][:, start + b : start + b + 1], (TILE, LANES))
                for t in range(home, count)
            }
            for b in range(group)
        ]
        rows = [tiles[home][at + a : at + a + 1, :] for a in range(group)]
        entry = [
            [col[b][home][at + a : at + a + 1, :] for b in range(a + 1)] for a in range(group)
        ]
        low = [[None] * group for _ in range(group)]
        inv = [[None] * group for _ in range(group)]
        for b in range(group):
            pivot = entry[b][b]
            for c in range(b):
                pivot = pivot - low[b][c] * low[b][c]
            root = lax.rsqrt(pivot)
            inv[b][b] = root
            for a in range(b + 1, group):
                value = entry[a][b]
                for c in range(b):
                    value = value - low[a][c] * low[b][c]
                low[a][b] = value * root
        for a in range(group):
            for b in range(a):
                value = low[a][b] * inv[b][b]
                for c in range(b + 1, a):
                    value = value + low[a][c] * inv[c][b]
                inv[a][b] = -(inv[a][a] * value)
        scaled = []
        for a in range(group):
            value = inv[a][0] * rows[0]
            for b in range(1, a + 1):
                value = value + inv[a][b] * rows[b]
            scaled.append(value)
        for t in range(home, count):
            if t == home and at + group == TILE:
                new = tiles[t]
            else:
                new = tiles[t]
                for a in range(group):
                    factor = inv[a][0] * col[0][t]
                    for b in range(1, a + 1):
                        factor = factor + inv[a][b] * col[b][t]
                    new = new - factor * scaled[a]
                if t == home:
                    new = jnp.where(row >= at + group, new, tiles[t])
            if t == home:
                for a in range(group):
                    new = jnp.where(row == at + a, scaled[a], new)
            tiles[t] = new
    return tiles


def factor_kernel(scale, nb, mine_ref, other_ref, w_ref, wh_ref, work, side):
    size = w_ref.shape[0]
    half = size // 2
    for k, part in enumerate(in_order(lax.axis_index("blk") % 2, mine_ref[...], other_ref[...])):
        work[k * half : (k + 1) * half, :size] = part[:, :size] * scale
        side[k * half : (k + 1) * half, :] = part[:, size:]
    row = lax.broadcasted_iota(jnp.int32, (size, size), 0)
    col = lax.broadcasted_iota(jnp.int32, (size, size), 1)
    work[:, size:] = (row == col).astype(F32)
    small_row = lax.broadcasted_iota(jnp.int32, (nb, nb), 0)
    small_col = lax.broadcasted_iota(jnp.int32, (nb, nb), 1)
    unit = (small_row == small_col).astype(F32)
    for k in range(size // nb):
        low, high = k * nb, (k + 1) * nb
        both = jnp.concatenate([work[low:high, low:high], unit], axis=1)
        tiles = eliminate([both[t * TILE : (t + 1) * TILE, :] for t in range(nb // TILE)], nb)
        own = jnp.concatenate(tiles, axis=0)[:, nb : 2 * nb]
        wide = dot_three(own, work[low:high, :])
        w_ref[low:high, :] = wide[:, size:]
        if high < size:
            left = wide[:, high:size].T
            work[high:, :] = work[high:, :] - dot_three(left, wide)
    wh_ref[...] = dot_three(w_ref[...], side[...])


def factor_inverse(mine, other, scale):
    size = 2 * mine.shape[0]
    rest = mine.shape[1] - size
    return local_call(
        functools.partial(factor_kernel, scale, LANES // 2),
        [VMEM, VMEM],
        [jax.ShapeDtypeStruct((size, size), F32), jax.ShapeDtypeStruct((size, rest), F32)],
        [VMEM, VMEM],
        scratch_shapes=[pltpu.VMEM((size, 2 * size), F32), pltpu.VMEM((size, rest), F32)],
    )(mine, other)


def flip(x, masks):
    return lax.ppermute(x, "blk", [(i, i ^ m) for i, m in enumerate(masks)])


def sum_steps(total):
    bits = [1 << k for k in range(1, total.bit_length() - 1)]
    return [
        [bits[k] if i % 2 == 0 else bits[-1 - k] for i in range(total)] for k in range(len(bits))
    ]


def body(
    panel_column, upper_inverse, panel_rows, trailing, sketch, row_map, parent_block, parent_slot
):
    blk_count = lax.axis_size("blk")
    front_count = lax.axis_size("front")
    front_index = lax.axis_index("front")
    me = lax.axis_index("blk")
    trail = trailing[0]
    rows, cols = trail.shape
    per_device = row_map.shape[1]
    slab_rows = rows * blk_count
    own_cols = cols // blk_count
    own_panel = panel_rows[0]

    cores = [1] * blk_count
    steps = sum_steps(blk_count)

    own_sketch = lax.dynamic_slice_in_dim(sketch, me * own_cols, own_cols, 0)
    local = fdot(own_panel, own_sketch)
    half = local.shape[0] // 2
    away = lax.dynamic_slice_in_dim(local, (1 - me % 2) * half, half, 0)
    mine = lax.dynamic_slice_in_dim(local, (me % 2) * half, half, 0)
    came = flip(away, cores)
    mine = mine + came
    for step in steps:
        came = flip(mine, step)
        mine = mine + came
    other = flip(mine, cores)
    chunks = 8
    trail_sketch, kept, factored = sketch_part(
        0, chunks // 2, chunks, trail, sketch, panel_column[0], upper_inverse[0]
    )
    trail_sketch = sketch_part(
        chunks // 2, chunks // 2, chunks, trail, sketch, trail_sketch, kept
    )[0]
    sketched, turned, away, mine = finish_sketch(trail_sketch, kept, mine, other)

    colours = 2 if own_cols % (2 * LANES) == 0 else 1
    width = own_cols // colours
    others = [1 << k for k in range(1, blk_count.bit_length() - 1)]
    orders = [[1] + others, [1] + others[::-1]][:colours]
    stages = len(orders[0])
    came = flip(away, cores)
    mine = mine + came
    received = []
    jobs = [(colour, order, 0) for colour, order in enumerate(orders)]
    sent = share_product(jobs, colours, turned, trail, width, BF16)
    for colour in range(colours):
        received.append([flip(sent[colour], cores)])
    shares = [[] for _ in orders]
    for wanted in ([1], list(range(2, stages + 1))):
        jobs = [(c, order, stage) for c, order in enumerate(orders) for stage in wanted]
        got = share_product(jobs, colours, turned, trail, width, F32)
        for (colour, _, _), share in zip(jobs, got):
            shares[colour].append(share)
    kept_rows, away_rows = spread_rows(sketched, row_map[0], blk_count)
    kept_rows, away_rows = kept_rows[:, None], away_rows[:, None]
    reach = blk_count // 2
    distances = [0]
    while True:
        came_rows = flip(away_rows, [reach] * blk_count)
        if reach == 1:
            break
        kept_rows, away_rows = regroup(kept_rows, came_rows)
        distances += [d + reach for d in distances]
        reach //= 2
    distances += [d + 1 for d in distances]
    spread = [x.reshape((1, -1) + x.shape[3:]) for x in (kept_rows, came_rows)]
    for step in steps:
        came = flip(mine, step)
        mine = mine + came
    other = flip(mine, cores)

    def exchange(stage):
        for colour, order in enumerate(orders):
            sent = merge(order, stage, shares[colour][stage - 1], received[colour])
            received[colour].append(flip(sent, [order[stage]] * blk_count))

    exchange(1)
    inverse, inverse_products = factor_inverse(mine, other, 1.0 / slab_rows)

    parent_number = jnp.arange(parent_slot.shape[0], dtype=jnp.int32)
    own_blocks = lax.dynamic_index_in_dim(parent_block, front_index, 0, keepdims=False)
    owner = jnp.sum(
        jnp.where(own_blocks[:, None] == parent_number[None, :], parent_slot[None, :], 0), axis=1
    )
    device_number = jnp.arange(front_count * blk_count, dtype=jnp.int32)
    block_number = jnp.arange(blk_count * per_device, dtype=jnp.int32)
    rank_of = [distances.index(d) for d in range(blk_count)]
    distance = jnp.bitwise_xor(block_number // per_device, me)
    place = jnp.sum(
        jnp.where(
            distance[:, None] == jnp.arange(blk_count, dtype=jnp.int32)[None, :],
            jnp.array(rank_of, jnp.int32)[None, :],
            0,
        ),
        axis=1,
    )
    block_number = place * per_device + block_number % per_device + 1
    source = jnp.sum(
        jnp.where(owner[None, :] == device_number[:, None], block_number[None, :], 0), axis=1
    ).astype(jnp.int32)
    outgoing = route_left(source, spread, inverse)
    incoming = lax.all_to_all(outgoing, ("front", "blk"), 0, 0, tiled=True)

    for stage in range(2, stages):
        exchange(stage)
    early = right_early(
        orders,
        inverse,
        inverse_products,
        own_panel,
        [share[-1] for share in shares],
        [group[:-1] for group in received],
    )
    right = right_late(
        inverse, early, [group[-1] for group in received], 1.0 / math.sqrt(slab_rows)
    )
    parent_rows = gather_left(incoming, front_count)
    return (factored[None], right[None], parent_rows)


def solution(mesh):
    return jax.shard_map(
        body,
        mesh=mesh,
        in_specs=(
            P("front", "blk", None),
            P("front", None, None),
            P("front", None, "blk"),
            P("front", "blk", None),
            P(),
            P("front", "blk", None),
            P(),
            P(),
        ),
        out_specs=(
            P("front", "blk", None),
            P("front", "blk", None),
            P(("front", "blk"), None),
        ),
        check_vma=False,
    )
```
